32 devices in a mesh: blk: 4 (over x, core), uly: 8 (over z, y).
Axes of the slice: x: 2, y: 2, z: 4, core: 2. Of those that a mesh axis runs over, the one named last changes fastest.
Arguments:
- query: bfloat16 [4096, 4096], P(('blk', 'uly')), may hold values from -5 to 5
- key_input: bfloat16 [4096, 512], P(('blk', 'uly')), may hold values from -5 to 5
- value_input: bfloat16 [4096, 512], P(('blk', 'uly')), may hold values from -6 to 6
- output: bfloat16 [4096, 4096], P(('blk', 'uly')), may hold values from -6 to 6
- out_grad: bfloat16 [4096, 4096], P(('blk', 'uly')), may hold values from -6 to 6
Outputs:
- query_grad: bfloat16 [4096, 4096], P(('blk', 'uly'))
- key_gradient: bfloat16 [4096, 512], P(('blk', 'uly'))
- value_gradient: bfloat16 [4096, 512], P(('blk', 'uly'))
The draws below stay inside these ranges and needn't reach their ends.
All inputs are finite; a program needn't handle non-finite values.
Results may differ from the reference program's by a relative error of at most 0.009.
Values may be sent and summed in bfloat16 or wider, within the bound.
A program may use at most 64 MiB of HBM per device.

```python
import jax
import jax.numpy as jnp
from jax import lax

QUERY_HEADS = 32
KEY_VALUE_HEADS = 4
HEAD_SIZE = 128
WINDOW_KEYS = 1024
SEQUENCE_TOKENS = 4096


def draw_query(key, part):
    start_offset = jnp.clip(jax.random.normal(jax.random.fold_in(key, 1), (SEQUENCE_TOKENS, QUERY_HEADS * HEAD_SIZE), jnp.float32), -5.0, 5.0)
    return start_offset.astype(jnp.bfloat16)


def draw_key_input(key, part):
    start_offset = jnp.clip(jax.random.normal(jax.random.fold_in(key, 5), (SEQUENCE_TOKENS, KEY_VALUE_HEADS * HEAD_SIZE), jnp.float32), -5.0, 5.0)
    return start_offset.astype(jnp.bfloat16)


def block_scale(key, extent, pieces, least, top_value):
    loudness, own = 1.0, jax.random.fold_in(key, 6)
    for position, parts in pieces:
        heights = jnp.exp(jax.random.uniform(jax.random.fold_in(own, position), (parts,), jnp.float32, least / len(pieces), top_value / len(pieces)))
        loudness = loudness * jnp.repeat(heights, extent[position] // parts).reshape([-1 if axis == position else 1 for axis in range(len(extent))])
    return loudness


def gaussian(key, shape, scale, limit, cuts=(), kind=jnp.bfloat16):
    drawn = jax.random.normal(key, shape, jnp.float32) * scale
    if len(cuts) > 0:
        drawn = block_scale(key, shape, cuts, -0.22, 0.18) * drawn
    return jnp.clip(drawn, min=-limit, max=limit).astype(kind)


def setup_inputs(seed: int = 0) -> dict:
    streams_of = jax.random.split(jax.random.key(seed), 6)
    query = draw_query(jax.random.fold_in(streams_of[5], 71), 0)
    key_input = draw_key_input(jax.random.fold_in(streams_of[5], 71), 0)
    value_input = gaussian(streams_of[2], (SEQUENCE_TOKENS, KEY_VALUE_HEADS * HEAD_SIZE), 1.0, 6.0, ((0, 32),))
    output = gaussian(streams_of[3], (SEQUENCE_TOKENS, QUERY_HEADS * HEAD_SIZE), 1.0, 6.0, ((0, 32),))
    out_grad = gaussian(streams_of[4], (SEQUENCE_TOKENS, QUERY_HEADS * HEAD_SIZE), 1.0, 6.0, ((0, 32),))
    return dict(query=query, key_input=key_input, value_input=value_input, output=output, out_grad=out_grad)


def reference(query, key_input, value_input, output, out_grad):
    scaling = HEAD_SIZE ** -0.5
    group_width = QUERY_HEADS // KEY_VALUE_HEADS
    block = min(512, SEQUENCE_TOKENS)
    block_count = SEQUENCE_TOKENS // block
    span = WINDOW_KEYS + block
    highest = lax.Precision.HIGHEST
    query_heads = query.reshape(SEQUENCE_TOKENS, QUERY_HEADS, HEAD_SIZE).transpose(1, 0, 2)
    output_heads = output.reshape(SEQUENCE_TOKENS, QUERY_HEADS, HEAD_SIZE).transpose(1, 0, 2)
    grad_heads = out_grad.reshape(SEQUENCE_TOKENS, QUERY_HEADS, HEAD_SIZE).transpose(1, 0, 2)
    key_head_rows = jnp.pad(key_input.reshape(SEQUENCE_TOKENS, KEY_VALUE_HEADS, HEAD_SIZE).transpose(1, 0, 2), ((0, 0), (WINDOW_KEYS, 0), (0, 0)))
    value_head_rows = jnp.pad(value_input.reshape(SEQUENCE_TOKENS, KEY_VALUE_HEADS, HEAD_SIZE).transpose(1, 0, 2), ((0, 0), (WINDOW_KEYS, 0), (0, 0)))
    offsets = jnp.arange(block, dtype=jnp.int32)[:, None]
    columns = jnp.arange(span, dtype=jnp.int32)[None, :]
    relative = columns - offsets
    inside = (relative >= 1) & (relative <= WINDOW_KEYS)

    def group_member_count(group):
        key_pad = key_head_rows[group].astype(jnp.float32)
        value_pad = value_head_rows[group].astype(jnp.float32)

        def per_head(carry, member):
            key_acc, value_acc = carry
            head = group * group_width + member
            query_wide = query_heads[head].astype(jnp.float32)
            grad_wide = grad_heads[head].astype(jnp.float32)
            row_dot = jnp.sum(output_heads[head].astype(jnp.float32) * grad_wide, axis=1)

            def per_block(inner, index):
                key_acc, value_acc = inner
                start = (index * block).astype(jnp.int32)
                query_block = lax.dynamic_slice_in_dim(query_wide, start, block, 0)
                grad_block = lax.dynamic_slice_in_dim(grad_wide, start, block, 0)
                dot_block = lax.dynamic_slice_in_dim(row_dot, start, block, 0)
                key_block = lax.dynamic_slice_in_dim(key_pad, start, span, 0)
                value_block = lax.dynamic_slice_in_dim(value_pad, start, span, 0)
                visible = inside & (start - WINDOW_KEYS + columns >= 0)
                scores = jnp.dot(query_block, key_block.T, precision=highest) * scaling
                masked = jnp.where(visible, scores, -1e30)
                row_max = jnp.max(masked, axis=1)
                row_sum = jnp.sum(jnp.where(visible, jnp.exp(masked - row_max[:, None]), 0.0), axis=1)
                log_total = row_max + jnp.log(row_sum)
                weights = jnp.where(visible, jnp.exp(masked - log_total[:, None]), 0.0)
                weights_low = weights.astype(jnp.bfloat16).astype(jnp.float32)
                weight_grad = jnp.dot(grad_block, value_block.T, precision=highest)
                score_grad = (weights * (weight_grad - dot_block[:, None]) * scaling).astype(jnp.bfloat16)
                score_wide = score_grad.astype(jnp.float32)
                query_portion = jnp.dot(score_wide, key_block, precision=highest)
                key_portion = jnp.dot(score_wide.T, query_block, precision=highest)
                value_portion = jnp.dot(weights_low.T, grad_block, precision=highest)
                key_acc = lax.dynamic_update_slice_in_dim(
                    key_acc, lax.dynamic_slice_in_dim(key_acc, start, span, 0) + key_portion, start, 0)
                value_acc = lax.dynamic_update_slice_in_dim(
                    value_acc, lax.dynamic_slice_in_dim(value_acc, start, span, 0) + value_portion, start, 0)
                return (key_acc, value_acc), query_portion

            (key_acc, value_acc), query_parts = lax.scan(
                per_block, (key_acc, value_acc), jnp.arange(block_count, dtype=jnp.int32))
            return (key_acc, value_acc), query_parts.reshape(SEQUENCE_TOKENS, HEAD_SIZE).astype(jnp.bfloat16)

        zeros = jnp.zeros((SEQUENCE_TOKENS + WINDOW_KEYS, HEAD_SIZE), jnp.float32)
        (key_acc, value_acc), query_portion = lax.scan(
            per_head, (zeros, zeros), jnp.arange(group_width, dtype=jnp.int32))
        return query_portion, key_acc[WINDOW_KEYS:], value_acc[WINDOW_KEYS:]

    query_portion, key_portion, value_portion = lax.map(group_member_count, jnp.arange(KEY_VALUE_HEADS, dtype=jnp.int32))
    query_grad = query_portion.reshape(QUERY_HEADS, SEQUENCE_TOKENS, HEAD_SIZE).transpose(1, 0, 2).reshape(SEQUENCE_TOKENS, QUERY_HEADS * HEAD_SIZE)
    key_gradient = key_portion.transpose(1, 0, 2).reshape(SEQUENCE_TOKENS, KEY_VALUE_HEADS * HEAD_SIZE).astype(jnp.bfloat16)
    value_gradient = value_portion.transpose(1, 0, 2).reshape(SEQUENCE_TOKENS, KEY_VALUE_HEADS * HEAD_SIZE).astype(jnp.bfloat16)
    return (query_grad, key_gradient, value_gradient)
```

```python
import functools
import math

import jax
import jax.numpy as jnp
from jax import lax
from jax.experimental import pallas as pl
from jax.experimental.pallas import tpu as pltpu
from jax.sharding import PartitionSpec as P

QUERY_HEADS = 32
KEY_VALUE_HEADS = 4
HEAD_SIZE = 128
WINDOW_KEYS = 1024
GROUP = QUERY_HEADS // KEY_VALUE_HEADS
PAIRS = GROUP // 2
AHEAD = 6
HOME_LAG = 1
FINISH_LAG = 6
WIDTH = 2
WIDE_GATHER = 1
WIDE_REDUCE = 0
WIDE_HOPS = ((0, 1, 3, 5),)
WIDE_LAG = 0
WIDE_GAP = 1
DIRECT = 0
EARLY = 3
SECOND = 0
WIDE_FIRST = -1
MESH = pl.DeviceIdType.MESH
F32 = jnp.float32
BF16 = jnp.bfloat16
NT = (((1,), (1,)), ((), ()))
TN = (((0,), (0,)), ((), ()))


def kernel(
    rows, back, blks, ulys,
    q_hbm, k_hbm, v_hbm, o_hbm, g_hbm,
    dq_hbm, dk_ref, dv_ref,
    dq_ref, q_ref, o_ref, g_ref, kv, acc_k, acc_v, pair_send, pair_recv, home_send, home_recv,
    relay_recv, load_sem, kv_sem, far_ss, far_rs, near_ss, near_rs, gn_ss, gn_rs, gf_ss, gf_rs,
    on_ss, rl_rs, ws_send, ws_recv, wl_send, wl_recv,
    wp_ss, wp_rs, wc_ss, wc_rs, gw_ss, gw_rs, gl_ss, gl_rs,
):
    half = back // 2
    heads = KEY_VALUE_HEADS
    scaling = HEAD_SIZE ** (-0.5)
    total = blks * ulys
    me = lax.axis_index("blk") * ulys + lax.axis_index("uly")
    par = lax.rem(me, 2)
    partner = me + 1 - 2 * par
    level = lax.rem(me, back) // 2
    up, down = me + 2, me - 2

    def where_is(t):
        return (t // ulys, lax.rem(t, ulys))

    loads = [
        pltpu.make_async_copy(s, d, load_sem.at[i])
        for i, (s, d) in enumerate(((q_hbm, q_ref), (o_hbm, o_ref), (g_hbm, g_ref)))
    ]
    dq_out = [pltpu.make_async_copy(dq_ref, dq_hbm, load_sem.at[3])]
    kv_loads = []
    for h in range(heads):
        for i, src in enumerate((k_hbm, v_hbm)):
            kv_loads.append(
                pltpu.make_async_copy(
                    src.at[:, h * HEAD_SIZE : (h + 1) * HEAD_SIZE], kv.at[h, back + 1, i], kv_sem.at[h, i]
                )
            )
    for copy in kv_loads:
        copy.start()
    for copy in loads:
        copy.start()

    def loop(count, fn):
        def body(i, carry):
            fn(i)
            return carry

        lax.fori_loop(0, count, body, 0)

    barrier = pltpu.get_barrier_semaphore()

    def greet(k):
        for there, peer in ((me + 2 * k + 2 < total, me + 2 * k + 2), (me - 2 * k - 2 >= 0, me - 2 * k - 2)):

            @pl.when(there)
            def _():
                pl.semaphore_signal(barrier, inc=1, device_id=where_is(peer), device_id_type=MESH)

    loop(half, greet)
    pl.semaphore_signal(barrier, inc=1, device_id=where_is(partner), device_id_type=MESH)

    @pl.when(me < back)
    def _():
        def clear(s):
            @pl.when(me - back + s < 0)
            def _():
                for h in range(heads):
                    kv[h, s + 1] = jnp.zeros((2, rows, HEAD_SIZE), BF16)

        loop(back, clear)

    later, earlier = (total - 1 - me) // 2, me // 2
    pl.semaphore_wait(barrier, 1 + jnp.minimum(later, half) + jnp.minimum(earlier, half))

    def remote(src, dst, ss, rs, target):
        return pltpu.make_async_remote_copy(
            src_ref=src, dst_ref=dst, send_sem=ss, recv_sem=rs,
            device_id=where_is(target), device_id_type=MESH,
        )

    def far(h, k):
        return remote(
            kv.at[h, back + 1], kv.at[h, back + 1 - 2 * k], far_ss.at[h, k - 1], far_rs.at[h, k - 1], me + 2 * k
        )

    def near(h, k):
        return remote(
            kv.at[h, back + 1 - 2 * k - 2 * par], kv.at[h, back - 2 * k],
            near_ss.at[h, k], near_rs.at[h, k], partner,
        )

    rises = (level >= 2) & (level < half - 1)
    falls = (me >= back) & (level > 0) & (level + 2 < half)

    def far_out(k, h=None):
        away = jnp.where(level + k < half, k, half - k)
        straight = away != 3
        if h is not None:
            straight = straight | (h < DIRECT)
        return (me + 2 * k < total) & straight

    def onward(h, k, to, target):
        return remote(
            kv.at[h, back + 1 - 2 * k], kv.at[h, back + 1 - 2 * to], on_ss.at[h], far_rs.at[h, to - 1], target
        )

    def turn(q):
        top = jnp.where(q < 2, half - 1 + q, half - q)
        inner = jnp.where(q < 2, half - q, q - 1)
        return jnp.where(level == half - 1, top, jnp.where(level == 0, q + 1, inner))

    def far_in(k):
        return me - 2 * k >= 0

    def near_out(k):
        return me - 2 * k - 2 * par >= 0

    def near_in(k):
        return me - 1 - 2 * k >= 0

    def send_own(h):
        def one(i):
            k = half - i

            @pl.when(far_out(k, h))
            def _():
                far(h, k).start()

        loop(half, one)

        @pl.when(par == 0)
        def _():
            near(h, 0).start()

    def hand_on(h, k):
        @pl.when(far_in(k))
        def _():
            far(h, k).wait_recv()

            @pl.when((k == 2) & rises & (h >= DIRECT))
            def _():
                onward(h, k, k + 1, up).start()

            @pl.when((k == half - 2) & falls & (h >= DIRECT))
            def _():
                onward(h, k, k - 1, down).start()

            @pl.when(k - par < half)
            def _():
                near(h, k - par).start()

    def gather_finish(h):
        def one(k):
            @pl.when(near_in(k))
            def _():
                near(h, k).wait_recv()

        loop(half, one)

    def gn(h, k):
        return remote(pair_send.at[h, k], pair_recv.at[h, k], gn_ss.at[h, k], gn_rs.at[h, k], partner)

    def gf(h, k):
        return remote(
            home_send.at[h, k - 1], home_recv.at[h, k - 1], gf_ss.at[h, k - 1], gf_rs.at[h, k - 1],
            me - 2 * k,
        )

    def reduce_pair(h, k):
        pair_send[h, k, 0] = (acc_k[h, back - 2 * k] * scaling).astype(BF16)
        pair_send[h, k, 1] = acc_v[h, back - 2 * k].astype(BF16)

        @pl.when(near_in(k))
        def _():
            gn(h, k).start()

    def relay(h, k, target):
        return remote(home_send.at[h, k - 1], relay_recv.at[h], gf_ss.at[h, k - 1], rl_rs.at[h], target)

    def reduce_home(h, k):
        n = k - par
        at = back + 1 - 2 * k
        rise = (k == 3) & (k <= level)
        fall = (k == half - 3) & (k > level)

        @pl.when(far_in(k))
        def _():
            @pl.when(n < half)
            def _():
                gn(h, n).wait_recv()

            @pl.when(((k == 2) & rises) | ((k == half - 2) & falls))
            def _():
                relay(h, k, up).wait_recv()
                acc_k[h, at] += relay_recv[h, 0].astype(F32) * (1.0 / scaling)
                acc_v[h, at] += relay_recv[h, 1].astype(F32)

            @pl.when(n < half)
            def _():
                home_send[h, k - 1, 0] = (acc_k[h, at] * scaling + pair_recv[h, n, 0].astype(F32)).astype(BF16)
                home_send[h, k - 1, 1] = (acc_v[h, at] + pair_recv[h, n, 1].astype(F32)).astype(BF16)

            @pl.when(n == half)
            def _():
                home_send[h, k - 1, 0] = (acc_k[h, at] * scaling).astype(BF16)
                home_send[h, k - 1, 1] = acc_v[h, at].astype(BF16)

            @pl.when(rise)
            def _():
                relay(h, k, down).start()

            @pl.when(fall)
            def _():
                relay(h, k, up).start()

            @pl.when(jnp.logical_not(rise | fall))
            def _():
                gf(h, k).start()

    def reduce_finish(h):
        acc_k[h, back + 1] = acc_k[h, back + 1] * scaling

        @pl.when(par == 0)
        def _():
            gn(h, 0).wait_recv()
            acc_k[h, back + 1] += pair_recv[h, 0, 0].astype(F32)
            acc_v[h, back + 1] += pair_recv[h, 0, 1].astype(F32)

        def one(i):
            k = i + 1

            @pl.when(far_out(k))
            def _():
                gf(h, k).wait_recv()
                acc_k[h, back + 1] += home_recv[h, i, 0].astype(F32)
                acc_v[h, back + 1] += home_recv[h, i, 1].astype(F32)

        loop(half, one)
        columns = pl.ds(pl.multiple_of(h * HEAD_SIZE, HEAD_SIZE), HEAD_SIZE)
        dk_ref[:, columns] = acc_k[h, back + 1].astype(BF16)
        dv_ref[:, columns] = acc_v[h, back + 1].astype(BF16)

    has_up, has_down = level < half - 1, level > 0
    after, before = me + back, me - back
    has_after, has_before = after < total, before >= 0

    def two_at(k):
        return pl.ds(back + 1 - 2 * k - par, 2)

    def wide_pair(h, w):
        return remote(
            kv.at[h, back + 1], kv.at[h, back + 2 * par], wp_ss.at[w], wp_rs.at[w], partner
        )

    def wide_chain(h, w, k, to, target, s):
        return remote(
            kv.at[h, two_at(k)], kv.at[h, two_at(to)], wc_ss.at[w, s], wc_rs.at[w, to], target
        )

    def wide_start(h, w):
        wide_pair(h, w).wait_recv()

        @pl.when(has_after)
        def _():
            wide_chain(h, w, 0, half, after, half + 1).start()

        @pl.when(has_up)
        def _():
            wide_chain(h, w, 0, 1, up, 0).start()

    def wide_hop(h, w, n):
        @pl.when(n <= level)
        def _():
            wide_chain(h, w, n - 1, n, down, 0).wait_recv()

            @pl.when(has_up)
            def _():
                wide_chain(h, w, n, n + 1, up, n).start()

        k = half + 1 - n

        @pl.when(has_before & (k > level))
        def _():
            wide_chain(h, w, 0, k, up, 0).wait_recv()

            @pl.when(has_down)
            def _():
                wide_chain(h, w, k, k - 1, down, k).start()

    def wide_sum(w, e, to, target):
        return remote(ws_send.at[w, e], ws_recv.at[w, to], gw_ss.at[w, e], gw_rs.at[w, to], target)

    def wide_last(w):
        return remote(wl_send.at[w], wl_recv.at[w], gl_ss.at[w], gl_rs.at[w], partner)

    def wide_step(h, w, j):
        @pl.when(j == 0)
        def _():
            acc_k[h] = acc_k[h] * scaling

        def take(slot, at):
            acc_k[h, at] += ws_recv[w, slot, 0].astype(F32)
            acc_v[h, at] += ws_recv[w, slot, 1].astype(F32)

        def pack(e):
            ws_send[w, e, 0] = acc_k[h, two_at(e)].astype(BF16)
            ws_send[w, e, 1] = acc_v[h, two_at(e)].astype(BF16)

        e = half - 1 - j

        @pl.when((e <= level) & (e >= 0))
        def _():
            @pl.when(has_up)
            def _():
                wide_sum(w, 0, e, up).wait_recv()
                take(e, two_at(e))

            @pl.when(e > 0)
            def _():
                pack(e)
                wide_sum(w, e, e - 1, down).start()

        f = j + 1

        @pl.when(has_before & (f > level) & (f <= half))
        def _():
            @pl.when(has_down)
            def _():
                wide_sum(w, 0, f, down).wait_recv()
                take(f, two_at(f))

            pack(f)

            @pl.when(f < half)
            def _():
                wide_sum(w, f, f + 1, up).start()

            @pl.when(f == half)
            def _():
                wide_sum(w, f, half + 1, before).start()

        @pl.when(j == half)
        def _():
            @pl.when(has_after)
            def _():
                wide_sum(w, 0, half + 1, after).wait_recv()
                take(half + 1, two_at(0))

            other = back + 2 - 2 * par
            wl_send[w, 0] = acc_k[h, other].astype(BF16)
            wl_send[w, 1] = acc_v[h, other].astype(BF16)
            wide_last(w).start()

        @pl.when(j == half + 1)
        def _():
            wide_last(w).wait_recv()
            columns = slice(h * HEAD_SIZE, (h + 1) * HEAD_SIZE)
            dk_ref[:, columns] = (acc_k[h, back + 1] + wl_recv[w, 0].astype(F32)).astype(BF16)
            dv_ref[:, columns] = (acc_v[h, back + 1] + wl_recv[w, 1].astype(F32)).astype(BF16)

    def compute(h, p):
        first = pl.multiple_of((h * GROUP + 2 * p) * HEAD_SIZE, HEAD_SIZE)
        second = pl.multiple_of(first + HEAD_SIZE, HEAD_SIZE)

        def two(ref):
            return jnp.concatenate(
                [ref[:, pl.ds(first, HEAD_SIZE)], ref[:, pl.ds(second, HEAD_SIZE)]], axis=0
            )

        q2, g2, o2 = two(q_ref), two(g_ref), two(o_ref)
        rd = jnp.sum((o2.astype(F32) * g2.astype(F32)).T, axis=0, keepdims=True)
        keys = kv[h, 1 : back + 2, 0].reshape((back + 1) * rows, HEAD_SIZE)
        values = kv[h, 1 : back + 2, 1].reshape((back + 1) * rows, HEAD_SIZE)
        st = lax.dot_general(keys, q2, NT, preferred_element_type=F32)
        dp = lax.dot_general(values, g2, NT, preferred_element_type=F32)
        key_at = lax.broadcasted_iota(jnp.int32, (rows, 2 * rows), 0)
        query_at = lax.rem(lax.broadcasted_iota(jnp.int32, (rows, 2 * rows), 1), rows)
        tri = key_at > query_at
        gone = [jnp.where(me - back + s < 0, 1e30, 0.0).astype(F32) for s in range(back)]

        def cut(a, s):
            return a[s * rows : (s + 1) * rows]

        c = scaling * math.log2(math.e)
        blocks = [jnp.where(tri, cut(st, 0) - gone[0], cut(st, back))]
        blocks += [cut(st, s) for s in range(1, back)]
        top = jnp.max(blocks[0], axis=0, keepdims=True)
        for s in range(1, back):
            top = jnp.maximum(top, jnp.max(blocks[s], axis=0, keepdims=True) - gone[s])
        top = top * c
        probs = [jnp.exp2(blocks[0] * c - top)]
        probs += [jnp.exp2(blocks[s] * c - (top + gone[s])) for s in range(1, back)]
        sums = jnp.sum(probs[0], axis=0, keepdims=True)
        for s in range(1, back):
            sums = sums + jnp.sum(probs[s], axis=0, keepdims=True)
        inv = 1.0 / sums
        dps = [jnp.where(tri, cut(dp, 0), cut(dp, back))] + [cut(dp, s) for s in range(1, back)]
        ws = [a * inv for a in probs]
        ds = [w * (a - rd) for w, a in zip(ws, dps)]

        def spread(parts):
            low = [jnp.where(tri, parts[0], 0.0)] + parts[1:] + [jnp.where(tri, 0.0, parts[0])]
            return jnp.concatenate([a.astype(BF16) for a in low], axis=0)

        wt, dst = spread(ws), spread(ds)
        shape = (back + 1, rows, HEAD_SIZE)
        acc_v[h, 1 : back + 2] += jnp.dot(wt, g2, preferred_element_type=F32).reshape(shape)
        acc_k[h, 1 : back + 2] += jnp.dot(dst, q2, preferred_element_type=F32).reshape(shape)
        dq = lax.dot_general(dst, keys, TN, preferred_element_type=F32) * scaling
        dq_ref[:, pl.ds(first, HEAD_SIZE)] = dq[:rows].astype(BF16)
        dq_ref[:, pl.ds(second, HEAD_SIZE)] = dq[rows:].astype(BF16)

    narrow = heads - WIDE_GATHER
    for h in range(heads):
        kv_loads[2 * h].wait()
        kv_loads[2 * h + 1].wait()

        if h < EARLY:
            send_own(h)
        elif h >= narrow:
            wide_pair(h, h - narrow).start()


    order = half - 1
    per = PAIRS // WIDTH
    count = heads * per
    each = half // per

    def hand_on_at(f):
        @pl.when(f < narrow * half)
        def _():
            hand_on(f // half, lax.rem(lax.rem(f, half) + order, half) + 1)

    acc_k[...] = jnp.zeros_like(acc_k)
    acc_v[...] = jnp.zeros_like(acc_v)
    loop(SECOND, hand_on_at)
    for h in range(EARLY, narrow):
        send_own(h)
    loop(half + AHEAD - SECOND, lambda f: hand_on_at(f + SECOND))
    if WIDE_FIRST < 0:
        for w in range(WIDE_GATHER):
            wide_start(narrow + w, w)
    for copy in loads:
        copy.wait()

    def drain_gather(h):
        @pl.when((rises | falls) & (h >= DIRECT))
        def _():
            onward(h, 0, 1, up).wait_send()

        def inner(i):
            @pl.when(far_out(i + 1, h))
            def _():
                far(h, i + 1).wait_send()

            @pl.when(near_out(i))
            def _():
                near(h, i).wait_send()

        loop(half, inner)

    def sent():
        loop(narrow, drain_gather)
        for w in range(WIDE_GATHER):
            h = narrow + w
            wide_pair(h, w).wait_send()

            @pl.when(has_up)
            def _():
                wide_chain(h, w, 0, 1, up, 0).wait_send()

            @pl.when(has_after)
            def _():
                wide_chain(h, w, 0, half, after, half + 1).wait_send()

            def inner(i):
                n = i + 1

                @pl.when((has_up & (n <= level)) | (has_down & has_before & (n > level)))
                def _():
                    wide_chain(h, w, n, n - 1, down, n).wait_send()

            loop(half, inner)

    def piece(c):
        h, i = c // per, lax.rem(c, per)

        @pl.when((c < narrow * per) & (i == 0))
        def _():
            gather_finish(h)

        @pl.when(c < count)
        def _():
            for n in range(WIDTH):
                compute(h, i * WIDTH + n)

        @pl.when((c >= WIDE_REDUCE * per) & (c < count) & (i == per - 1))
        def _():
            def one(q):
                n = turn(q) - 1 + par
                reduce_pair(h, jnp.where(n < half, n, 0))

            loop(half, one)

        loop(each, lambda n: hand_on_at(c * each + n + half + AHEAD))

        def home_at(n):
            late = (c - per) * each + n - HOME_LAG
            g = jnp.maximum(late, 0) // half

            @pl.when((late >= 0) & (g >= WIDE_REDUCE) & (g < heads))
            def _():
                reduce_home(g, turn(lax.rem(late, half)))

        loop(each, home_at)
        @pl.when(c == count)
        def _():
            sent()
            for copy in dq_out:
                copy.start()

        late = c - 2 * per - FINISH_LAG
        e = jnp.maximum(late, 0) // per

        @pl.when((late >= 0) & (e >= WIDE_REDUCE) & (e < heads) & (lax.rem(late, per) == 0))
        def _():
            reduce_finish(e)

        for w in range(WIDE_GATHER):
            if WIDE_FIRST >= 0:

                @pl.when(c == WIDE_FIRST)
                def _():
                    wide_start(narrow + w, w)

            for n, at in enumerate(WIDE_HOPS[w]):

                @pl.when(c == at)
                def _():
                    wide_hop(narrow + w, w, n + 1)

        for w in range(WIDE_REDUCE):
            step = c - (w + 1) * per + 1 - WIDE_LAG
            j = jnp.maximum(step, 0) // WIDE_GAP

            @pl.when((step >= 0) & (j < half + 2) & (j * WIDE_GAP == step))
            def _():
                wide_step(w, w, j)

    narrow_end = count + per + 1 + max(HOME_LAG, FINISH_LAG + per)
    wide_end = WIDE_REDUCE * per + WIDE_LAG + WIDE_GAP * (half + 1)
    loop(max(narrow_end, wide_end), piece)

    def drain_reduce(h):
        def inner(i):
            @pl.when(near_in(i))
            def _():
                gn(h, i).wait_send()

            @pl.when(far_in(i + 1))
            def _():
                gf(h, i + 1).wait_send()

        loop(half, inner)

    for copy in dq_out:
        copy.wait()
    loop(heads - WIDE_REDUCE, lambda i: drain_reduce(i + WIDE_REDUCE))
    for w in range(WIDE_REDUCE):
        wide_last(w).wait_send()

        def inner(i):
            n = i + 1

            @pl.when((n <= level) | has_before)
            def _():
                wide_sum(w, n, n - 1, down).wait_send()

        loop(half, inner)


def local(query, key_input, value_input, output, out_grad):
    rows, width = query.shape
    blks, ulys = lax.axis_size("blk"), lax.axis_size("uly")
    back = WINDOW_KEYS // rows
    half = back // 2
    heads = KEY_VALUE_HEADS
    one = (rows, HEAD_SIZE)
    pair = (2,) + one
    dma = pltpu.SemaphoreType.DMA
    vmem = pltpu.VMEM
    any_spec = pl.BlockSpec(memory_space=pl.ANY)
    vmem_spec = pl.BlockSpec(memory_space=vmem)
    return pl.pallas_call(
        functools.partial(kernel, rows, back, blks, ulys),
        out_shape=(
            jax.ShapeDtypeStruct(query.shape, BF16),
            jax.ShapeDtypeStruct(key_input.shape, BF16),
            jax.ShapeDtypeStruct(value_input.shape, BF16),
        ),
        in_specs=[any_spec] * 5,
        out_specs=(any_spec, vmem_spec, vmem_spec),
        scratch_shapes=[
            vmem((rows, width), BF16),
            vmem((rows, width), BF16),
            vmem((rows, width), BF16),
            vmem((rows, width), BF16),
            vmem((heads, back + 3) + pair, BF16),
            vmem((heads, back + 3) + one, F32),
            vmem((heads, back + 3) + one, F32),
            vmem((heads, half) + pair, BF16),
            vmem((heads, half) + pair, BF16),
            vmem((heads, half) + pair, BF16),
            vmem((heads, half) + pair, BF16),
            vmem((heads,) + pair, BF16),
            dma((4,)),
            dma((heads, 2)),
        ]
        + [dma((heads, half))] * 8
        + [dma((heads,))] * 2
        + [vmem((max(WIDE_REDUCE, 1), half + 2, 2, 2) + one, BF16)] * 2
        + [vmem((max(WIDE_REDUCE, 1), 2) + one, BF16)] * 2
        + [dma((max(WIDE_GATHER, 1),))] * 2
        + [dma((max(WIDE_GATHER, 1), half + 2))] * 2
        + [dma((max(WIDE_REDUCE, 1), half + 2))] * 2
        + [dma((max(WIDE_REDUCE, 1),))] * 2,
        compiler_params=pltpu.CompilerParams(
            collective_id=0, has_side_effects=True, vmem_limit_bytes=60 * 1024 * 1024
        ),
    )(query, key_input, value_input, output, out_grad)


def solution(mesh):
    spec = P(("blk", "uly"), None)
    return jax.shard_map(
        local, mesh=mesh, in_specs=(spec,) * 5, out_specs=(spec,) * 3, check_vma=False
    )
```

```python
import functools
import math

import jax
import jax.numpy as jnp
from jax import lax
from jax.experimental import pallas as pl
from jax.experimental.pallas import tpu as pltpu
from jax.sharding import PartitionSpec as P

QUERY_HEADS = 32
KEY_VALUE_HEADS = 4
HEAD_SIZE = 128
WINDOW_KEYS = 1024
GROUP = QUERY_HEADS // KEY_VALUE_HEADS
PAIRS = GROUP // 2
AHEAD = 4
HOME_LAG = 2
FINISH_LAG = 5
WIDTH = 2
WIDE_GATHER = 1
WIDE_REDUCE = 1
WIDE_HOPS = ((-1,0,2,4,5),)
WIDE_STEPS = ((2,4,9,10),)
SEND_ORDER = lambda i, half: half - i
DIRECT = 0
EARLY = 3
SECOND = 0
MESH = pl.DeviceIdType.MESH
F32 = jnp.float32
BF16 = jnp.bfloat16
NT = (((1,), (1,)), ((), ()))
TN = (((0,), (0,)), ((), ()))


def kernel(
    rows, back, blks, ulys,
    q_hbm, k_hbm, v_hbm, o_hbm, g_hbm,
    dq_hbm, dk_hbm, dv_hbm,
    dq_ref, dk_ref, dv_ref, dots, q_ref, o_ref, g_ref, kv, acc_k, acc_v, pair_send, pair_recv, home_send, home_recv,
    relay_recv, load_sem, kv_sem, far_ss, far_rs, near_ss, near_rs, gn_ss, gn_rs, gf_ss, gf_rs,
    on_ss, rl_rs, out_sem, ws_send, ws_recv, wl_send, wl_recv,
    wp_ss, wp_rs, wc_ss, wc_rs, gw_ss, gw_rs, gl_ss, gl_rs,
):
    half = back // 2
    heads = KEY_VALUE_HEADS
    scaling = HEAD_SIZE ** (-0.5)
    total = blks * ulys
    me = lax.axis_index("blk") * ulys + lax.axis_index("uly")
    par = lax.rem(me, 2)
    partner = me + 1 - 2 * par
    level = lax.rem(me, back) // 2
    up, down = me + 2, me - 2

    def where_is(t):
        return (t // ulys, lax.rem(t, ulys))

    loads = [
        pltpu.make_async_copy(s, d, load_sem.at[i])
        for i, (s, d) in enumerate(((q_hbm, q_ref), (o_hbm, o_ref), (g_hbm, g_ref)))
    ]
    dq_out = [pltpu.make_async_copy(dq_ref, dq_hbm, load_sem.at[3])]
    kv_loads = []
    for h in range(heads):
        for i, src in enumerate((k_hbm, v_hbm)):
            kv_loads.append(
                pltpu.make_async_copy(
                    src.at[:, h * HEAD_SIZE : (h + 1) * HEAD_SIZE], kv.at[h, back + 1, i], kv_sem.at[h, i]
                )
            )
    for copy in kv_loads:
        copy.start()
    for copy in loads:
        copy.start()

    def loop(count, fn):
        def body(i, carry):
            fn(i)
            return carry

        lax.fori_loop(0, count, body, 0)

    barrier = pltpu.get_barrier_semaphore()

    def greet(k):
        for there, peer in ((me + 2 * k + 2 < total, me + 2 * k + 2), (me - 2 * k - 2 >= 0, me - 2 * k - 2)):

            @pl.when(there)
            def _():
                pl.semaphore_signal(barrier, inc=1, device_id=where_is(peer), device_id_type=MESH)

    loop(half, greet)
    pl.semaphore_signal(barrier, inc=1, device_id=where_is(partner), device_id_type=MESH)

    @pl.when(me < back)
    def _():
        def clear(s):
            @pl.when(me - back + s < 0)
            def _():
                for h in range(heads):
                    kv[h, s + 1] = jnp.zeros((2, rows, HEAD_SIZE), BF16)

        loop(back, clear)

    later, earlier = (total - 1 - me) // 2, me // 2
    pl.semaphore_wait(barrier, 1 + jnp.minimum(later, half) + jnp.minimum(earlier, half))

    def remote(src, dst, ss, rs, target):
        return pltpu.make_async_remote_copy(
            src_ref=src, dst_ref=dst, send_sem=ss, recv_sem=rs,
            device_id=where_is(target), device_id_type=MESH,
        )

    def far(h, k):
        return remote(
            kv.at[h, back + 1], kv.at[h, back + 1 - 2 * k], far_ss.at[h, k - 1], far_rs.at[h, k - 1], me + 2 * k
        )

    def near(h, k):
        return remote(
            kv.at[h, back + 1 - 2 * k - 2 * par], kv.at[h, back - 2 * k],
            near_ss.at[h, k], near_rs.at[h, k], partner,
        )

    rises = (level >= 2) & (level < half - 1)
    falls = (me >= back) & (level > 0) & (level + 2 < half)

    def far_out(k, h=None):
        away = jnp.where(level + k < half, k, half - k)
        straight = away != 3
        if h is not None:
            straight = straight | (h < DIRECT)
        return (me + 2 * k < total) & straight

    def onward(h, k, to, target):
        return remote(
            kv.at[h, back + 1 - 2 * k], kv.at[h, back + 1 - 2 * to], on_ss.at[h], far_rs.at[h, to - 1], target
        )

    def turn(q):
        top = jnp.where(q < 2, half - 1 + q, half - q)
        inner = jnp.where(q < 2, half - q, q - 1)
        return jnp.where(level == half - 1, top, jnp.where(level == 0, q + 1, inner))

    def arrival(q):
        inner = jnp.where(q < 2, q, half + 1 - q)
        there = jnp.where(level == half - 1, q, jnp.where(level == 0, half - q, inner))
        return jnp.where(q == 0, half, there)

    def far_in(k):
        return me - 2 * k >= 0

    def near_out(k):
        return me - 2 * k - 2 * par >= 0

    def near_in(k):
        return me - 1 - 2 * k >= 0

    def send_own(h):
        def one(i):
            k = SEND_ORDER(i, half)

            @pl.when(far_out(k, h))
            def _():
                far(h, k).start()

        loop(half, one)

        @pl.when(par == 0)
        def _():
            near(h, 0).start()

    def hand_on(h, k):
        @pl.when(far_in(k))
        def _():
            far(h, k).wait_recv()

            @pl.when((k == 2) & rises & (h >= DIRECT))
            def _():
                onward(h, k, k + 1, up).start()

            @pl.when((k == half - 2) & falls & (h >= DIRECT))
            def _():
                onward(h, k, k - 1, down).start()

            @pl.when(k - par < half)
            def _():
                near(h, k - par).start()

    def gather_finish(h):
        def one(k):
            @pl.when(near_in(k))
            def _():
                near(h, k).wait_recv()

        loop(half, one)

    def gn(h, k):
        return remote(pair_send.at[h, k], pair_recv.at[h, k], gn_ss.at[h, k], gn_rs.at[h, k], partner)

    def gf(h, k):
        return remote(
            home_send.at[h, k - 1], home_recv.at[h, k - 1], gf_ss.at[h, k - 1], gf_rs.at[h, k - 1],
            me - 2 * k,
        )

    def reduce_pair(h, k):
        pair_send[h, k, 0] = (acc_k[h, back - 2 * k] * scaling).astype(BF16)
        pair_send[h, k, 1] = acc_v[h, back - 2 * k].astype(BF16)

        @pl.when(near_in(k))
        def _():
            gn(h, k).start()

    def relay(h, k, target):
        return remote(home_send.at[h, k - 1], relay_recv.at[h], gf_ss.at[h, k - 1], rl_rs.at[h], target)

    def reduce_home(h, k):
        n = k - par
        at = back + 1 - 2 * k
        rise = (k == 3) & (k <= level)
        fall = (k == half - 3) & (k > level)

        @pl.when(far_in(k))
        def _():
            @pl.when(n < half)
            def _():
                gn(h, n).wait_recv()

            @pl.when(((k == 2) & rises) | ((k == half - 2) & falls))
            def _():
                relay(h, k, up).wait_recv()
                acc_k[h, at] += relay_recv[h, 0].astype(F32) * (1.0 / scaling)
                acc_v[h, at] += relay_recv[h, 1].astype(F32)

            @pl.when(n < half)
            def _():
                home_send[h, k - 1, 0] = (acc_k[h, at] * scaling + pair_recv[h, n, 0].astype(F32)).astype(BF16)
                home_send[h, k - 1, 1] = (acc_v[h, at] + pair_recv[h, n, 1].astype(F32)).astype(BF16)

            @pl.when(n == half)
            def _():
                home_send[h, k - 1, 0] = (acc_k[h, at] * scaling).astype(BF16)
                home_send[h, k - 1, 1] = acc_v[h, at].astype(BF16)

            @pl.when(rise)
            def _():
                relay(h, k, down).start()

            @pl.when(fall)
            def _():
                relay(h, k, up).start()

            @pl.when(jnp.logical_not(rise | fall))
            def _():
                gf(h, k).start()

    def reduce_finish(h):
        acc_k[h, back + 1] = acc_k[h, back + 1] * scaling

        @pl.when(par == 0)
        def _():
            gn(h, 0).wait_recv()
            acc_k[h, back + 1] += pair_recv[h, 0, 0].astype(F32)
            acc_v[h, back + 1] += pair_recv[h, 0, 1].astype(F32)

        def one(i):
            k = i + 1

            @pl.when(far_out(k))
            def _():
                gf(h, k).wait_recv()
                acc_k[h, back + 1] += home_recv[h, i, 0].astype(F32)
                acc_v[h, back + 1] += home_recv[h, i, 1].astype(F32)

        loop(half, one)
        columns = pl.ds(pl.multiple_of(h * HEAD_SIZE, HEAD_SIZE), HEAD_SIZE)
        dk_ref[:, columns] = acc_k[h, back + 1].astype(BF16)
        dv_ref[:, columns] = acc_v[h, back + 1].astype(BF16)

    has_up, has_down = level < half - 1, level > 0
    after, before = me + back, me - back
    has_after, has_before = after < total, before >= 0

    def two_at(k):
        return pl.ds(back + 1 - 2 * k - par, 2)

    def wide_pair(h, w):
        return remote(
            kv.at[h, back + 1], kv.at[h, back + 2 * par], wp_ss.at[w], wp_rs.at[w], partner
        )

    def wide_chain(h, w, k, to, target, s):
        return remote(
            kv.at[h, two_at(k)], kv.at[h, two_at(to)], wc_ss.at[w, s], wc_rs.at[w, to], target
        )

    def wide_start(h, w):
        wide_pair(h, w).wait_recv()

        @pl.when(has_after)
        def _():
            wide_chain(h, w, 0, half, after, half + 1).start()

        @pl.when(has_up)
        def _():
            wide_chain(h, w, 0, 1, up, 0).start()

    def wide_hop(h, w, n):
        @pl.when(n <= level)
        def _():
            wide_chain(h, w, n - 1, n, down, 0).wait_recv()

            @pl.when(has_up)
            def _():
                wide_chain(h, w, n, n + 1, up, n).start()

        k = half + 1 - n

        @pl.when(has_before & (k > level))
        def _():
            wide_chain(h, w, 0, k, up, 0).wait_recv()

            @pl.when(has_down)
            def _():
                wide_chain(h, w, k, k - 1, down, k).start()

    def wide_sum(w, e, to, target):
        return remote(ws_send.at[w, e], ws_recv.at[w, to], gw_ss.at[w, e], gw_rs.at[w, to], target)

    def wide_last(w):
        return remote(wl_send.at[w], wl_recv.at[w], gl_ss.at[w], gl_rs.at[w], partner)

    def wide_relay(w, k, target):
        return remote(
            ws_send.at[w, k], ws_recv.at[w, half + 1], gw_ss.at[w, k], gw_rs.at[w, half + 1], target
        )

    def wide_step(h, w, j):
        def take(slot, at):
            acc_k[h, at] += ws_recv[w, slot, 0].astype(F32)
            acc_v[h, at] += ws_recv[w, slot, 1].astype(F32)

        def send(k):
            ws_send[w, k, 0] = acc_k[h, two_at(k)].astype(BF16)
            ws_send[w, k, 1] = acc_v[h, two_at(k)].astype(BF16)
            rise = (k == 3) & (k <= level)
            fall = (k == half - 3) & (k > level)

            @pl.when(rise)
            def _():
                wide_relay(w, k, down).start()

            @pl.when(fall)
            def _():
                wide_relay(w, k, up).start()

            @pl.when(jnp.logical_not(rise | fall))
            def _():
                wide_sum(w, k, k, me - 2 * k).start()

        def joins(k):
            return ((k == 2) & rises) | ((k == half - 2) & falls)

        @pl.when(j == 0)
        def _():
            acc_k[h] = acc_k[h] * scaling

            def one(q):
                k = turn(q)

                @pl.when(far_in(k) & jnp.logical_not(joins(k)))
                def _():
                    send(k)

            loop(half, one)

        @pl.when((j == 1) & (rises | falls))
        def _():
            k = jnp.where(rises, 2, half - 2)
            wide_relay(w, 0, up).wait_recv()
            take(half + 1, two_at(k))
            send(k)

        @pl.when(j == 2)
        def _():
            def one(i):
                @pl.when(far_out(i + 1))
                def _():
                    wide_sum(w, 0, i + 1, up).wait_recv()
                    take(i + 1, two_at(0))

            loop(half, one)
            other = back + 2 - 2 * par
            wl_send[w, 0] = acc_k[h, other].astype(BF16)
            wl_send[w, 1] = acc_v[h, other].astype(BF16)
            wide_last(w).start()

        @pl.when(j == 3)
        def _():
            wide_last(w).wait_recv()
            columns = slice(h * HEAD_SIZE, (h + 1) * HEAD_SIZE)
            dk_ref[:, columns] = (acc_k[h, back + 1] + wl_recv[w, 0].astype(F32)).astype(BF16)
            dv_ref[:, columns] = (acc_v[h, back + 1] + wl_recv[w, 1].astype(F32)).astype(BF16)

    def dot_rows(n):
        first = pl.multiple_of(2 * n * HEAD_SIZE, HEAD_SIZE)
        for i in range(2):
            at = pl.ds(pl.multiple_of(first + i * HEAD_SIZE, HEAD_SIZE), HEAD_SIZE)
            product = o_ref[:, at].astype(F32) * g_ref[:, at].astype(F32)
            dots[n, :, i * rows : (i + 1) * rows] = jnp.sum(product.T, axis=0, keepdims=True)

    def compute(h, p):
        first = pl.multiple_of((h * GROUP + 2 * p) * HEAD_SIZE, HEAD_SIZE)
        second = pl.multiple_of(first + HEAD_SIZE, HEAD_SIZE)

        def two(ref):
            return jnp.concatenate(
                [ref[:, pl.ds(first, HEAD_SIZE)], ref[:, pl.ds(second, HEAD_SIZE)]], axis=0
            )

        q2, g2 = two(q_ref), two(g_ref)
        rd = dots[h * PAIRS + p]
        keys = kv[h, 1 : back + 2, 0].reshape((back + 1) * rows, HEAD_SIZE)
        values = kv[h, 1 : back + 2, 1].reshape((back + 1) * rows, HEAD_SIZE)
        st = lax.dot_general(keys, q2, NT, preferred_element_type=F32)
        dp = lax.dot_general(values, g2, NT, preferred_element_type=F32)
        key_at = lax.broadcasted_iota(jnp.int32, (rows, 2 * rows), 0)
        query_at = lax.rem(lax.broadcasted_iota(jnp.int32, (rows, 2 * rows), 1), rows)
        tri = key_at > query_at
        gone = [jnp.where(me - back + s < 0, 1e30, 0.0).astype(F32) for s in range(back)]

        def cut(a, s):
            return a[s * rows : (s + 1) * rows]

        c = scaling * math.log2(math.e)
        blocks = [jnp.where(tri, cut(st, 0) - gone[0], cut(st, back))]
        blocks += [cut(st, s) for s in range(1, back)]
        top = jnp.max(blocks[0], axis=0, keepdims=True)
        for s in range(1, back):
            top = jnp.maximum(top, jnp.max(blocks[s], axis=0, keepdims=True) - gone[s])
        top = top * c
        probs = [jnp.exp2(blocks[0] * c - top)]
        probs += [jnp.exp2(blocks[s] * c - (top + gone[s])) for s in range(1, back)]
        sums = jnp.sum(probs[0], axis=0, keepdims=True)
        for s in range(1, back):
            sums = sums + jnp.sum(probs[s], axis=0, keepdims=True)
        inv = 1.0 / sums
        dps = [jnp.where(tri, cut(dp, 0), cut(dp, back))] + [cut(dp, s) for s in range(1, back)]
        ws = [a * inv for a in probs]
        ds = [w * (a - rd) for w, a in zip(ws, dps)]

        def spread(parts):
            low = [jnp.where(tri, parts[0], 0.0)] + parts[1:] + [jnp.where(tri, 0.0, parts[0])]
            return jnp.concatenate([a.astype(BF16) for a in low], axis=0)

        wt, dst = spread(ws), spread(ds)
        shape = (back + 1, rows, HEAD_SIZE)
        acc_v[h, 1 : back + 2] += jnp.dot(wt, g2, preferred_element_type=F32).reshape(shape)
        acc_k[h, 1 : back + 2] += jnp.dot(dst, q2, preferred_element_type=F32).reshape(shape)
        dq = lax.dot_general(dst, keys, TN, preferred_element_type=F32) * scaling
        dq_ref[:, pl.ds(first, HEAD_SIZE)] = dq[:rows].astype(BF16)
        dq_ref[:, pl.ds(second, HEAD_SIZE)] = dq[rows:].astype(BF16)

    narrow = heads - WIDE_GATHER
    for h in range(heads):
        kv_loads[2 * h].wait()
        kv_loads[2 * h + 1].wait()

        if h < EARLY:
            send_own(h)
        elif h >= narrow:
            wide_pair(h, h - narrow).start()


    per = PAIRS // WIDTH
    count = heads * per
    each = half // per

    def hand_on_at(f):
        @pl.when(f < narrow * half)
        def _():
            hand_on(f // half, arrival(lax.rem(f, half)))

    acc_k[...] = jnp.zeros_like(acc_k)
    acc_v[...] = jnp.zeros_like(acc_v)
    for copy in loads:
        copy.wait()
    loop(heads * PAIRS, dot_rows)
    loop(SECOND, hand_on_at)
    for h in range(EARLY, narrow):
        send_own(h)
    reached = SECOND
    events = sorted(
        (at, w, n) for w in range(WIDE_GATHER) for n, at in enumerate(WIDE_HOPS[w]) if at < 0
    )
    for at, w, n in events:
        upto = half + AHEAD + at + 1
        if upto > reached:
            loop(upto - reached, lambda f, first=reached: hand_on_at(f + first))
            reached = upto
        if n == 0:
            wide_start(narrow + w, w)
        else:
            wide_hop(narrow + w, w, n)
    loop(half + AHEAD - reached, lambda f: hand_on_at(f + reached))
    def drain_gather(h):
        @pl.when((rises | falls) & (h >= DIRECT))
        def _():
            onward(h, 0, 1, up).wait_send()

        def inner(i):
            @pl.when(far_out(i + 1, h))
            def _():
                far(h, i + 1).wait_send()

            @pl.when(near_out(i))
            def _():
                near(h, i).wait_send()

        loop(half, inner)

    def sent():
        loop(narrow, drain_gather)
        for w in range(WIDE_GATHER):
            h = narrow + w
            wide_pair(h, w).wait_send()

            @pl.when(has_up)
            def _():
                wide_chain(h, w, 0, 1, up, 0).wait_send()

            @pl.when(has_after)
            def _():
                wide_chain(h, w, 0, half, after, half + 1).wait_send()

            def inner(i):
                n = i + 1

                @pl.when((has_up & (n <= level)) | (has_down & has_before & (n > level)))
                def _():
                    wide_chain(h, w, n, n - 1, down, n).wait_send()

            loop(half, inner)

    def results(h):
        columns = pl.ds(pl.multiple_of(h * HEAD_SIZE, HEAD_SIZE), HEAD_SIZE)
        return [
            pltpu.make_async_copy(s.at[:, columns], d.at[:, columns], out_sem.at[i, h])
            for i, (s, d) in enumerate(((dk_ref, dk_hbm), (dv_ref, dv_hbm)))
        ]

    def drain_reduce(h):
        def inner(i):
            @pl.when(near_in(i))
            def _():
                gn(h, i).wait_send()

            @pl.when(far_in(i + 1))
            def _():
                gf(h, i + 1).wait_send()

        loop(half, inner)

    def piece(c):
        h, i = c // per, lax.rem(c, per)

        @pl.when((c < narrow * per) & (i == 0))
        def _():
            gather_finish(h)

        @pl.when(c < count)
        def _():
            for n in range(WIDTH):
                compute(h, i * WIDTH + n)

        @pl.when((c >= WIDE_REDUCE * per) & (c < count) & (i == per - 1))
        def _():
            def one(q):
                n = turn(q) - 1 + par
                reduce_pair(h, jnp.where(n < half, n, 0))

            loop(half, one)

        loop(each, lambda n: hand_on_at(c * each + n + half + AHEAD))

        def home_at(n):
            late = (c - per) * each + n - HOME_LAG
            g = jnp.maximum(late, 0) // half

            @pl.when((late >= 0) & (g >= WIDE_REDUCE) & (g < heads))
            def _():
                reduce_home(g, turn(lax.rem(late, half)))

        loop(each, home_at)
        @pl.when(c == count)
        def _():
            sent()
            for copy in dq_out:
                copy.start()

        late = c - 2 * per - FINISH_LAG
        e = jnp.maximum(late, 0) // per

        @pl.when((late >= 0) & (e >= WIDE_REDUCE) & (e < heads) & (lax.rem(late, per) == 0))
        def _():
            @pl.when(e == heads - 1)
            def _():
                loop(heads - 1 - WIDE_REDUCE, lambda i: drain_reduce(i + WIDE_REDUCE))

            reduce_finish(e)
            for copy in results(e):
                copy.start()

        for w in range(WIDE_GATHER):
            for n, at in enumerate(WIDE_HOPS[w]):
                if at >= 0:

                    @pl.when(c == at)
                    def _():
                        if n == 0:
                            wide_start(narrow + w, w)
                        else:
                            wide_hop(narrow + w, w, n)

        for w in range(WIDE_REDUCE):
            for j, at in enumerate(WIDE_STEPS[w]):

                @pl.when(c == at)
                def _():
                    wide_step(w, w, j)
                    if j == 3:
                        for copy in results(w):
                            copy.start()

    narrow_end = count + per + 1 + max(HOME_LAG, FINISH_LAG + per)
    loop(max(narrow_end, 1 + max(max(steps) for steps in WIDE_STEPS)), piece)

    for copy in dq_out:
        copy.wait()

    def done(h):
        for copy in results(h):
            copy.wait()

    loop(heads, done)
    drain_reduce(heads - 1)
    for w in range(WIDE_REDUCE):
        wide_last(w).wait_send()

        def inner(i):
            n = i + 1

            @pl.when((n <= level) | has_before)
            def _():
                wide_sum(w, n, n - 1, down).wait_send()

        loop(half, inner)


def local(query, key_input, value_input, output, out_grad):
    rows, width = query.shape
    blks, ulys = lax.axis_size("blk"), lax.axis_size("uly")
    back = WINDOW_KEYS // rows
    half = back // 2
    heads = KEY_VALUE_HEADS
    one = (rows, HEAD_SIZE)
    pair = (2,) + one
    dma = pltpu.SemaphoreType.DMA
    vmem = pltpu.VMEM
    any_spec = pl.BlockSpec(memory_space=pl.ANY)
    return pl.pallas_call(
        functools.partial(kernel, rows, back, blks, ulys),
        out_shape=(
            jax.ShapeDtypeStruct(query.shape, BF16),
            jax.ShapeDtypeStruct(key_input.shape, BF16),
            jax.ShapeDtypeStruct(value_input.shape, BF16),
        ),
        in_specs=[any_spec] * 5,
        out_specs=(any_spec,) * 3,
        scratch_shapes=[
            vmem((rows, width), BF16),
            vmem(key_input.shape, BF16),
            vmem(value_input.shape, BF16),
            vmem((heads * PAIRS, 1, 2 * rows), F32),
            vmem((rows, width), BF16),
            vmem((rows, width), BF16),
            vmem((rows, width), BF16),
            vmem((heads, back + 3) + pair, BF16),
            vmem((heads, back + 3) + one, F32),
            vmem((heads, back + 3) + one, F32),
            vmem((heads, half) + pair, BF16),
            vmem((heads, half) + pair, BF16),
            vmem((heads, half) + pair, BF16),
            vmem((heads, half) + pair, BF16),
            vmem((heads,) + pair, BF16),
            dma((4,)),
            dma((heads, 2)),
        ]
        + [dma((heads, half))] * 8
        + [dma((heads,))] * 2
        + [dma((2, heads))]
        + [vmem((max(WIDE_REDUCE, 1), half + 2, 2, 2) + one, BF16)] * 2
        + [vmem((max(WIDE_REDUCE, 1), 2) + one, BF16)] * 2
        + [dma((max(WIDE_GATHER, 1),))] * 2
        + [dma((max(WIDE_GATHER, 1), half + 2))] * 2
        + [dma((max(WIDE_REDUCE, 1), half + 2))] * 2
        + [dma((max(WIDE_REDUCE, 1),))] * 2,
        compiler_params=pltpu.CompilerParams(
            collective_id=0, has_side_effects=True, vmem_limit_bytes=60 * 1024 * 1024
        ),
    )(query, key_input, value_input, output, out_grad)


def solution(mesh):
    spec = P(("blk", "uly"), None)
    return jax.shard_map(
        local, mesh=mesh, in_specs=(spec,) * 5, out_specs=(spec,) * 3, check_vma=False
    )
```

```python
import functools
import math

import jax
import jax.numpy as jnp
from jax import lax
from jax.experimental import pallas as pl
from jax.experimental.pallas import tpu as pltpu
from jax.sharding import PartitionSpec as P

QUERY_HEADS = 32
KEY_VALUE_HEADS = 4
HEAD_SIZE = 128
WINDOW_KEYS = 1024
GROUP = QUERY_HEADS // KEY_VALUE_HEADS
PAIRS = GROUP // 2
AHEAD = 4
HOME_LAG = 2
FINISH_LAG = 5
WIDTH = 2
WIDE_GATHER = 1
WIDE_REDUCE = 1
WIDE_HOPS = ((-1,0,2,4,5),)
WIDE_STEPS = ((2,4,9,10),)
SEND_ORDER = lambda i, half: half - i
DIRECT = 0
EARLY = 2
SECOND = 1
MESH = pl.DeviceIdType.MESH
F32 = jnp.float32
BF16 = jnp.bfloat16
NT = (((1,), (1,)), ((), ()))
TN = (((0,), (0,)), ((), ()))


def kernel(
    rows, back, blks, ulys,
    q_hbm, k_hbm, v_hbm, o_hbm, g_hbm,
    dq_hbm, dk_hbm, dv_hbm,
    dq_ref, dk_ref, dv_ref, dots, q_ref, o_ref, g_ref, kv, acc_k, acc_v, pair_send, pair_recv, home_send, home_recv,
    relay_recv, load_sem, kv_sem, far_ss, far_rs, near_ss, near_rs, gn_ss, gn_rs, gf_ss, gf_rs,
    on_ss, rl_rs, out_sem, ws_send, ws_recv, wl_send, wl_recv,
    wp_ss, wp_rs, wc_ss, wc_rs, gw_ss, gw_rs, gl_ss, gl_rs,
):
    half = back // 2
    heads = KEY_VALUE_HEADS
    scaling = HEAD_SIZE ** (-0.5)
    total = blks * ulys
    me = lax.axis_index("blk") * ulys + lax.axis_index("uly")
    par = lax.rem(me, 2)
    partner = me + 1 - 2 * par
    level = lax.rem(me, back) // 2
    up, down = me + 2, me - 2

    def where_is(t):
        return (t // ulys, lax.rem(t, ulys))

    loads = [
        pltpu.make_async_copy(s, d, load_sem.at[i])
        for i, (s, d) in enumerate(((q_hbm, q_ref), (o_hbm, o_ref), (g_hbm, g_ref)))
    ]
    dq_out = [pltpu.make_async_copy(dq_ref, dq_hbm, load_sem.at[3])]
    kv_loads = []
    for h in range(heads):
        for i, src in enumerate((k_hbm, v_hbm)):
            kv_loads.append(
                pltpu.make_async_copy(
                    src.at[:, h * HEAD_SIZE : (h + 1) * HEAD_SIZE], kv.at[h, back + 1, i], kv_sem.at[h, i]
                )
            )
    for copy in kv_loads:
        copy.start()
    for copy in loads:
        copy.start()

    def loop(count, fn):
        def body(i, carry):
            fn(i)
            return carry

        lax.fori_loop(0, count, body, 0)

    barrier = pltpu.get_barrier_semaphore()

    def greet(k):
        for there, peer in ((me + 2 * k + 2 < total, me + 2 * k + 2), (me - 2 * k - 2 >= 0, me - 2 * k - 2)):

            @pl.when(there)
            def _():
                pl.semaphore_signal(barrier, inc=1, device_id=where_is(peer), device_id_type=MESH)

    loop(half, greet)
    pl.semaphore_signal(barrier, inc=1, device_id=where_is(partner), device_id_type=MESH)

    @pl.when(me < back)
    def _():
        def clear(s):
            @pl.when(me - back + s < 0)
            def _():
                for h in range(heads):
                    kv[h, s + 1] = jnp.zeros((2, rows, HEAD_SIZE), BF16)

        loop(back, clear)

    later, earlier = (total - 1 - me) // 2, me // 2
    pl.semaphore_wait(barrier, 1 + jnp.minimum(later, half) + jnp.minimum(earlier, half))

    def remote(src, dst, ss, rs, target):
        return pltpu.make_async_remote_copy(
            src_ref=src, dst_ref=dst, send_sem=ss, recv_sem=rs,
            device_id=where_is(target), device_id_type=MESH,
        )

    def far(h, k):
        return remote(
            kv.at[h, back + 1], kv.at[h, back + 1 - 2 * k], far_ss.at[h, k - 1], far_rs.at[h, k - 1], me + 2 * k
        )

    def near(h, k):
        return remote(
            kv.at[h, back + 1 - 2 * k - 2 * par], kv.at[h, back - 2 * k],
            near_ss.at[h, k], near_rs.at[h, k], partner,
        )

    rises = (level >= 2) & (level < half - 1)
    falls = (me >= back) & (level > 0) & (level + 2 < half)

    def far_out(k, h=None):
        away = jnp.where(level + k < half, k, half - k)
        straight = away != 3
        if h is not None:
            straight = straight | (h < DIRECT)
        return (me + 2 * k < total) & straight

    def onward(h, k, to, target):
        return remote(
            kv.at[h, back + 1 - 2 * k], kv.at[h, back + 1 - 2 * to], on_ss.at[h], far_rs.at[h, to - 1], target
        )

    def turn(q):
        top = jnp.where(q < 2, half - 1 + q, half - q)
        inner = jnp.where(q < 2, half - q, q - 1)
        return jnp.where(level == half - 1, top, jnp.where(level == 0, q + 1, inner))

    def arrival(q):
        inner = jnp.where(q < 2, q, half + 1 - q)
        there = jnp.where(level == half - 1, q, jnp.where(level == 0, half - q, inner))
        return jnp.where(q == 0, half, there)

    def far_in(k):
        return me - 2 * k >= 0

    def near_out(k):
        return me - 2 * k - 2 * par >= 0

    def near_in(k):
        return me - 1 - 2 * k >= 0

    def send_own(h):
        def one(i):
            k = SEND_ORDER(i, half)

            @pl.when(far_out(k, h))
            def _():
                far(h, k).start()

        loop(half, one)

        @pl.when(par == 0)
        def _():
            near(h, 0).start()

    def hand_on(h, k):
        @pl.when(far_in(k))
        def _():
            far(h, k).wait_recv()

            @pl.when((k == 2) & rises & (h >= DIRECT))
            def _():
                onward(h, k, k + 1, up).start()

            @pl.when((k == half - 2) & falls & (h >= DIRECT))
            def _():
                onward(h, k, k - 1, down).start()

            @pl.when(k - par < half)
            def _():
                near(h, k - par).start()

    def gather_finish(h):
        def one(k):
            @pl.when(near_in(k))
            def _():
                near(h, k).wait_recv()

        loop(half, one)

    def gn(h, k):
        return remote(pair_send.at[h, k], pair_recv.at[h, k], gn_ss.at[h, k], gn_rs.at[h, k], partner)

    def gf(h, k):
        return remote(
            home_send.at[h, k - 1], home_recv.at[h, k - 1], gf_ss.at[h, k - 1], gf_rs.at[h, k - 1],
            me - 2 * k,
        )

    def reduce_pair(h, k):
        pair_send[h, k, 0] = (acc_k[h, back - 2 * k] * scaling).astype(BF16)
        pair_send[h, k, 1] = acc_v[h, back - 2 * k].astype(BF16)

        @pl.when(near_in(k))
        def _():
            gn(h, k).start()

    def relay(h, k, target):
        return remote(home_send.at[h, k - 1], relay_recv.at[h], gf_ss.at[h, k - 1], rl_rs.at[h], target)

    def reduce_home(h, k):
        n = k - par
        at = back + 1 - 2 * k
        rise = (k == 3) & (k <= level)
        fall = (k == half - 3) & (k > level)

        @pl.when(far_in(k))
        def _():
            @pl.when(n < half)
            def _():
                gn(h, n).wait_recv()

            @pl.when(((k == 2) & rises) | ((k == half - 2) & falls))
            def _():
                relay(h, k, up).wait_recv()
                acc_k[h, at] += relay_recv[h, 0].astype(F32) * (1.0 / scaling)
                acc_v[h, at] += relay_recv[h, 1].astype(F32)

            @pl.when(n < half)
            def _():
                home_send[h, k - 1, 0] = (acc_k[h, at] * scaling + pair_recv[h, n, 0].astype(F32)).astype(BF16)
                home_send[h, k - 1, 1] = (acc_v[h, at] + pair_recv[h, n, 1].astype(F32)).astype(BF16)

            @pl.when(n == half)
            def _():
                home_send[h, k - 1, 0] = (acc_k[h, at] * scaling).astype(BF16)
                home_send[h, k - 1, 1] = acc_v[h, at].astype(BF16)

            @pl.when(rise)
            def _():
                relay(h, k, down).start()

            @pl.when(fall)
            def _():
                relay(h, k, up).start()

            @pl.when(jnp.logical_not(rise | fall))
            def _():
                gf(h, k).start()

    def reduce_finish(h):
        acc_k[h, back + 1] = acc_k[h, back + 1] * scaling

        @pl.when(par == 0)
        def _():
            gn(h, 0).wait_recv()
            acc_k[h, back + 1] += pair_recv[h, 0, 0].astype(F32)
            acc_v[h, back + 1] += pair_recv[h, 0, 1].astype(F32)

        def one(i):
            k = i + 1

            @pl.when(far_out(k))
            def _():
                gf(h, k).wait_recv()
                acc_k[h, back + 1] += home_recv[h, i, 0].astype(F32)
                acc_v[h, back + 1] += home_recv[h, i, 1].astype(F32)

        loop(half, one)
        columns = pl.ds(pl.multiple_of(h * HEAD_SIZE, HEAD_SIZE), HEAD_SIZE)
        dk_ref[:, columns] = acc_k[h, back + 1].astype(BF16)
        dv_ref[:, columns] = acc_v[h, back + 1].astype(BF16)

    has_up, has_down = level < half - 1, level > 0
    after, before = me + back, me - back
    has_after, has_before = after < total, before >= 0

    def two_at(k):
        return pl.ds(back + 1 - 2 * k - par, 2)

    def wide_pair(h, w):
        return remote(
            kv.at[h, back + 1], kv.at[h, back + 2 * par], wp_ss.at[w], wp_rs.at[w], partner
        )

    def wide_chain(h, w, k, to, target, s):
        return remote(
            kv.at[h, two_at(k)], kv.at[h, two_at(to)], wc_ss.at[w, s], wc_rs.at[w, to], target
        )

    def wide_start(h, w):
        wide_pair(h, w).wait_recv()

        @pl.when(has_after)
        def _():
            wide_chain(h, w, 0, half, after, half + 1).start()

        @pl.when(has_up)
        def _():
            wide_chain(h, w, 0, 1, up, 0).start()

    def wide_hop(h, w, n):
        @pl.when(n <= level)
        def _():
            wide_chain(h, w, n - 1, n, down, 0).wait_recv()

            @pl.when(has_up)
            def _():
                wide_chain(h, w, n, n + 1, up, n).start()

        k = half + 1 - n

        @pl.when(has_before & (k > level))
        def _():
            wide_chain(h, w, 0, k, up, 0).wait_recv()

            @pl.when(has_down)
            def _():
                wide_chain(h, w, k, k - 1, down, k).start()

    def wide_sum(w, e, to, target):
        return remote(ws_send.at[w, e], ws_recv.at[w, to], gw_ss.at[w, e], gw_rs.at[w, to], target)

    def wide_last(w):
        return remote(wl_send.at[w], wl_recv.at[w], gl_ss.at[w], gl_rs.at[w], partner)

    def wide_relay(w, k, target):
        return remote(
            ws_send.at[w, k], ws_recv.at[w, half + 1], gw_ss.at[w, k], gw_rs.at[w, half + 1], target
        )

    def wide_step(h, w, j):
        def take(slot, at):
            acc_k[h, at] += ws_recv[w, slot, 0].astype(F32)
            acc_v[h, at] += ws_recv[w, slot, 1].astype(F32)

        def send(k):
            ws_send[w, k, 0] = acc_k[h, two_at(k)].astype(BF16)
            ws_send[w, k, 1] = acc_v[h, two_at(k)].astype(BF16)
            rise = (k == 3) & (k <= level)
            fall = (k == half - 3) & (k > level)

            @pl.when(rise)
            def _():
                wide_relay(w, k, down).start()

            @pl.when(fall)
            def _():
                wide_relay(w, k, up).start()

            @pl.when(jnp.logical_not(rise | fall))
            def _():
                wide_sum(w, k, k, me - 2 * k).start()

        def joins(k):
            return ((k == 2) & rises) | ((k == half - 2) & falls)

        @pl.when(j == 0)
        def _():
            acc_k[h] = acc_k[h] * scaling

            def one(q):
                k = turn(q)

                @pl.when(far_in(k) & jnp.logical_not(joins(k)))
                def _():
                    send(k)

            loop(half, one)

        @pl.when((j == 1) & (rises | falls))
        def _():
            k = jnp.where(rises, 2, half - 2)
            wide_relay(w, 0, up).wait_recv()
            take(half + 1, two_at(k))
            send(k)

        @pl.when(j == 2)
        def _():
            def one(i):
                @pl.when(far_out(i + 1))
                def _():
                    wide_sum(w, 0, i + 1, up).wait_recv()
                    take(i + 1, two_at(0))

            loop(half, one)
            other = back + 2 - 2 * par
            wl_send[w, 0] = acc_k[h, other].astype(BF16)
            wl_send[w, 1] = acc_v[h, other].astype(BF16)
            wide_last(w).start()

        @pl.when(j == 3)
        def _():
            wide_last(w).wait_recv()
            columns = slice(h * HEAD_SIZE, (h + 1) * HEAD_SIZE)
            dk_ref[:, columns] = (acc_k[h, back + 1] + wl_recv[w, 0].astype(F32)).astype(BF16)
            dv_ref[:, columns] = (acc_v[h, back + 1] + wl_recv[w, 1].astype(F32)).astype(BF16)

    def dot_rows(n):
        first = pl.multiple_of(2 * n * HEAD_SIZE, HEAD_SIZE)
        for i in range(2):
            at = pl.ds(pl.multiple_of(first + i * HEAD_SIZE, HEAD_SIZE), HEAD_SIZE)
            product = o_ref[:, at].astype(F32) * g_ref[:, at].astype(F32)
            dots[n, :, i * rows : (i + 1) * rows] = jnp.sum(product.T, axis=0, keepdims=True)

    def compute(h, p):
        first = pl.multiple_of((h * GROUP + 2 * p) * HEAD_SIZE, HEAD_SIZE)
        second = pl.multiple_of(first + HEAD_SIZE, HEAD_SIZE)

        def two(ref):
            return jnp.concatenate(
                [ref[:, pl.ds(first, HEAD_SIZE)], ref[:, pl.ds(second, HEAD_SIZE)]], axis=0
            )

        q2, g2 = two(q_ref), two(g_ref)
        rd = dots[h * PAIRS + p]
        keys = kv[h, 1 : back + 2, 0].reshape((back + 1) * rows, HEAD_SIZE)
        values = kv[h, 1 : back + 2, 1].reshape((back + 1) * rows, HEAD_SIZE)
        st = lax.dot_general(keys, q2, NT, preferred_element_type=F32)
        dp = lax.dot_general(values, g2, NT, preferred_element_type=F32)
        key_at = lax.broadcasted_iota(jnp.int32, (rows, 2 * rows), 0)
        query_at = lax.rem(lax.broadcasted_iota(jnp.int32, (rows, 2 * rows), 1), rows)
        tri = key_at > query_at
        gone = [jnp.where(me - back + s < 0, 1e30, 0.0).astype(F32) for s in range(back)]

        def cut(a, s):
            return a[s * rows : (s + 1) * rows]

        c = scaling * math.log2(math.e)
        blocks = [jnp.where(tri, cut(st, 0) - gone[0], cut(st, back))]
        blocks += [cut(st, s) for s in range(1, back)]
        top = jnp.max(blocks[0], axis=0, keepdims=True)
        for s in range(1, back):
            top = jnp.maximum(top, jnp.max(blocks[s], axis=0, keepdims=True) - gone[s])
        top = top * c
        probs = [jnp.exp2(blocks[0] * c - top)]
        probs += [jnp.exp2(blocks[s] * c - (top + gone[s])) for s in range(1, back)]
        sums = jnp.sum(probs[0], axis=0, keepdims=True)
        for s in range(1, back):
            sums = sums + jnp.sum(probs[s], axis=0, keepdims=True)
        inv = 1.0 / sums
        dps = [jnp.where(tri, cut(dp, 0), cut(dp, back))] + [cut(dp, s) for s in range(1, back)]
        ws = [a * inv for a in probs]
        ds = [w * (a - rd) for w, a in zip(ws, dps)]

        def spread(parts):
            low = [jnp.where(tri, parts[0], 0.0)] + parts[1:] + [jnp.where(tri, 0.0, parts[0])]
            return jnp.concatenate([a.astype(BF16) for a in low], axis=0)

        wt, dst = spread(ws), spread(ds)
        shape = (back + 1, rows, HEAD_SIZE)
        acc_v[h, 1 : back + 2] += jnp.dot(wt, g2, preferred_element_type=F32).reshape(shape)
        acc_k[h, 1 : back + 2] += jnp.dot(dst, q2, preferred_element_type=F32).reshape(shape)
        dq = lax.dot_general(dst, keys, TN, preferred_element_type=F32) * scaling
        dq_ref[:, pl.ds(first, HEAD_SIZE)] = dq[:rows].astype(BF16)
        dq_ref[:, pl.ds(second, HEAD_SIZE)] = dq[rows:].astype(BF16)

    narrow = heads - WIDE_GATHER
    for h in range(heads):
        kv_loads[2 * h].wait()
        kv_loads[2 * h + 1].wait()

        if h < EARLY:
            send_own(h)
        elif h >= narrow:
            wide_pair(h, h - narrow).start()


    per = PAIRS // WIDTH
    count = heads * per
    each = half // per

    def hand_on_at(f):
        @pl.when(f < narrow * half)
        def _():
            hand_on(f // half, arrival(lax.rem(f, half)))

    acc_k[...] = jnp.zeros_like(acc_k)
    acc_v[...] = jnp.zeros_like(acc_v)
    for copy in loads:
        copy.wait()
    loop(heads * PAIRS, dot_rows)
    loop(SECOND, hand_on_at)
    for h in range(EARLY, narrow):
        send_own(h)
    reached = SECOND
    events = sorted(
        (at, w, n) for w in range(WIDE_GATHER) for n, at in enumerate(WIDE_HOPS[w]) if at < 0
    )
    for at, w, n in events:
        upto = half + AHEAD + at + 1
        if upto > reached:
            loop(upto - reached, lambda f, first=reached: hand_on_at(f + first))
            reached = upto
        if n == 0:
            wide_start(narrow + w, w)
        else:
            wide_hop(narrow + w, w, n)
    loop(half + AHEAD - reached, lambda f: hand_on_at(f + reached))
    def drain_gather(h):
        @pl.when((rises | falls) & (h >= DIRECT))
        def _():
            onward(h, 0, 1, up).wait_send()

        def inner(i):
            @pl.when(far_out(i + 1, h))
            def _():
                far(h, i + 1).wait_send()

            @pl.when(near_out(i))
            def _():
                near(h, i).wait_send()

        loop(half, inner)

    def sent():
        loop(narrow, drain_gather)
        for w in range(WIDE_GATHER):
            h = narrow + w
            wide_pair(h, w).wait_send()

            @pl.when(has_up)
            def _():
                wide_chain(h, w, 0, 1, up, 0).wait_send()

            @pl.when(has_after)
            def _():
                wide_chain(h, w, 0, half, after, half + 1).wait_send()

            def inner(i):
                n = i + 1

                @pl.when((has_up & (n <= level)) | (has_down & has_before & (n > level)))
                def _():
                    wide_chain(h, w, n, n - 1, down, n).wait_send()

            loop(half, inner)

    def results(h):
        columns = pl.ds(pl.multiple_of(h * HEAD_SIZE, HEAD_SIZE), HEAD_SIZE)
        return [
            pltpu.make_async_copy(s.at[:, columns], d.at[:, columns], out_sem.at[i, h])
            for i, (s, d) in enumerate(((dk_ref, dk_hbm), (dv_ref, dv_hbm)))
        ]

    def drain_reduce(h):
        def inner(i):
            @pl.when(near_in(i))
            def _():
                gn(h, i).wait_send()

            @pl.when(far_in(i + 1))
            def _():
                gf(h, i + 1).wait_send()

        loop(half, inner)

    def piece(c):
        h, i = c // per, lax.rem(c, per)

        @pl.when((c < narrow * per) & (i == 0))
        def _():
            gather_finish(h)

        @pl.when(c < count)
        def _():
            for n in range(WIDTH):
                compute(h, i * WIDTH + n)

        @pl.when((c >= WIDE_REDUCE * per) & (c < count) & (i == per - 1))
        def _():
            def one(q):
                n = turn(q) - 1 + par
                reduce_pair(h, jnp.where(n < half, n, 0))

            loop(half, one)

        loop(each, lambda n: hand_on_at(c * each + n + half + AHEAD))

        def home_at(n):
            late = (c - per) * each + n - HOME_LAG
            g = jnp.maximum(late, 0) // half

            @pl.when((late >= 0) & (g >= WIDE_REDUCE) & (g < heads))
            def _():
                reduce_home(g, turn(lax.rem(late, half)))

        loop(each, home_at)
        @pl.when(c == count)
        def _():
            sent()
            for copy in dq_out:
                copy.start()

        late = c - 2 * per - FINISH_LAG
        e = jnp.maximum(late, 0) // per

        @pl.when((late >= 0) & (e >= WIDE_REDUCE) & (e < heads) & (lax.rem(late, per) == 0))
        def _():
            @pl.when(e == heads - 1)
            def _():
                loop(heads - 1 - WIDE_REDUCE, lambda i: drain_reduce(i + WIDE_REDUCE))

            reduce_finish(e)
            for copy in results(e):
                copy.start()

        for w in range(WIDE_GATHER):
            for n, at in enumerate(WIDE_HOPS[w]):
                if at >= 0:

                    @pl.when(c == at)
                    def _():
                        if n == 0:
                            wide_start(narrow + w, w)
                        else:
                            wide_hop(narrow + w, w, n)

        for w in range(WIDE_REDUCE):
            for j, at in enumerate(WIDE_STEPS[w]):

                @pl.when(c == at)
                def _():
                    wide_step(w, w, j)
                    if j == 3:
                        for copy in results(w):
                            copy.start()

    narrow_end = count + per + 1 + max(HOME_LAG, FINISH_LAG + per)
    loop(max(narrow_end, 1 + max(max(steps) for steps in WIDE_STEPS)), piece)

    for copy in dq_out:
        copy.wait()

    def done(h):
        for copy in results(h):
            copy.wait()

    loop(heads, done)
    drain_reduce(heads - 1)
    for w in range(WIDE_REDUCE):
        wide_last(w).wait_send()

        def inner(i):
            n = i + 1

            @pl.when((n <= level) | has_before)
            def _():
                wide_sum(w, n, n - 1, down).wait_send()

        loop(half, inner)


def local(query, key_input, value_input, output, out_grad):
    rows, width = query.shape
    blks, ulys = lax.axis_size("blk"), lax.axis_size("uly")
    back = WINDOW_KEYS // rows
    half = back // 2
    heads = KEY_VALUE_HEADS
    one = (rows, HEAD_SIZE)
    pair = (2,) + one
    dma = pltpu.SemaphoreType.DMA
    vmem = pltpu.VMEM
    any_spec = pl.BlockSpec(memory_space=pl.ANY)
    return pl.pallas_call(
        functools.partial(kernel, rows, back, blks, ulys),
        out_shape=(
            jax.ShapeDtypeStruct(query.shape, BF16),
            jax.ShapeDtypeStruct(key_input.shape, BF16),
            jax.ShapeDtypeStruct(value_input.shape, BF16),
        ),
        in_specs=[any_spec] * 5,
        out_specs=(any_spec,) * 3,
        scratch_shapes=[
            vmem((rows, width), BF16),
            vmem(key_input.shape, BF16),
            vmem(value_input.shape, BF16),
            vmem((heads * PAIRS, 1, 2 * rows), F32),
            vmem((rows, width), BF16),
            vmem((rows, width), BF16),
            vmem((rows, width), BF16),
            vmem((heads, back + 3) + pair, BF16),
            vmem((heads, back + 3) + one, F32),
            vmem((heads, back + 3) + one, F32),
            vmem((heads, half) + pair, BF16),
            vmem((heads, half) + pair, BF16),
            vmem((heads, half) + pair, BF16),
            vmem((heads, half) + pair, BF16),
            vmem((heads,) + pair, BF16),
            dma((4,)),
            dma((heads, 2)),
        ]
        + [dma((heads, half))] * 8
        + [dma((heads,))] * 2
        + [dma((2, heads))]
        + [vmem((max(WIDE_REDUCE, 1), half + 2, 2, 2) + one, BF16)] * 2
        + [vmem((max(WIDE_REDUCE, 1), 2) + one, BF16)] * 2
        + [dma((max(WIDE_GATHER, 1),))] * 2
        + [dma((max(WIDE_GATHER, 1), half + 2))] * 2
        + [dma((max(WIDE_REDUCE, 1), half + 2))] * 2
        + [dma((max(WIDE_REDUCE, 1),))] * 2,
        compiler_params=pltpu.CompilerParams(
            collective_id=0, has_side_effects=True, vmem_limit_bytes=60 * 1024 * 1024
        ),
    )(query, key_input, value_input, output, out_grad)


def solution(mesh):
    spec = P(("blk", "uly"), None)
    return jax.shard_map(
        local, mesh=mesh, in_specs=(spec,) * 5, out_specs=(spec,) * 3, check_vma=False
    )
```
